32 devices in a mesh: groups: 2 (over x), expert: 16 (over z, y, core), beam: 1.
Axes of the slice: x: 2, y: 2, z: 4, core: 2. Of those that a mesh axis runs over, the one named last changes fastest.
Arguments:
- queries: bfloat16 [128, 2048], P(('groups', 'expert', 'beam')), parts along dimension 0, may hold values from -64 to 64
- new_keys: bfloat16 [128, 2048], P(('groups', 'expert', 'beam')), parts along dimension 0, may hold values from -4 to 4
- new_values: bfloat16 [128, 2048], P(('groups', 'expert', 'beam')), parts along dimension 0, may hold values from -4 to 4
- resid: bfloat16 [128, 2048], P(('groups', 'expert', 'beam')), parts along dimension 0, may hold values from -5 to 5
- key_cache: bfloat16 [128, 128, 2048], P(('groups', 'expert', 'beam')), parts along dimension 0, may hold values from -4 to 4
- value_cache: bfloat16 [128, 128, 2048], P(('groups', 'expert', 'beam')), parts along dimension 0, may hold values from -4 to 4
- parent: int32 [128], P('groups'), parts along dimension 0, may hold values from 0 to 63, as said below
- route_ids: int32 [128, 6], P('groups'), parts along dimension 0, may hold values from 0 to 15, all different within a row; in each aligned block of 4 rows (0 to 3, 4 to 7, ...) at most 2 rows name the same one
- route_weights: float32 [128, 6], P('groups'), parts along dimension 0, may hold values from 0.05 to 0.35
- norm_gain: float32 [2048], replicated, may hold values from 0.1 to 1.9
- w_gate: bfloat16 [16, 2048, 1408], P('expert', None, 'beam'), may hold values from -0.125 to 0.125
- w_up: bfloat16 [16, 2048, 1408], P('expert', None, 'beam'), may hold values from -0.125 to 0.125
- w_down: bfloat16 [16, 1408, 2048], P('expert', 'beam'), may hold values from -0.15625 to 0.15625
Outputs:
- layer_out: bfloat16 [128, 2048], P(('groups', 'expert', 'beam')), parts along dimension 0
The draws below stay inside these ranges and needn't reach their ends.
There are 2 independent parts, one for each index of `groups`. The reference program is written for one: setup_inputs(seed, part) draws one part's arguments, and reference() takes and returns one part's arrays. A program takes and returns all parts, laid end to end along the dimension named above; an argument that names none is the same for every part. Nothing has to cross between parts.
Inputs may be any that keep to these rules, and one draw needn't show every extreme that they name: `parent`: a permutation of 0 to 63. `route_ids`: the 6 experts of a slot differ; among the 4 slots of one device no expert is named by more than 2 slots, and this is reached.
All inputs are finite; a program needn't handle non-finite values.
Results may differ from the reference program's by a relative error of at most 0.0065.
Values may be sent and summed in bfloat16 or wider, within the bound.
A program may use at most 64 MiB of HBM per device.

```python
import math
import jax
import jax.numpy as jnp
import numpy as np
from jax import lax

HEADS = 16
HEAD_DIM = 128
D = 2048
FF = 1408
TOPK = 6
B_DEV = 4
CTX = 128
EXPERTS = 16
BEAMS = 64
CAP = 2


def beam_draws(key):
    parent = jax.random.permutation(jax.random.fold_in(key, 11), BEAMS).astype(jnp.int32)
    key_rows = jnp.clip(jax.random.normal(jax.random.fold_in(key, 12), (BEAMS, CTX, HEADS * HEAD_DIM), jnp.float32), -4.0, 4.0)
    query_rows = jnp.clip(jax.random.normal(jax.random.fold_in(key, 13), (BEAMS, HEADS * HEAD_DIM), jnp.float32), -4.0, 4.0)
    return (parent, key_rows, query_rows)


def draw_parent(key, part):
    return beam_draws(key)[0]


def draw_key_cache(key, part):
    return beam_draws(key)[1].astype(jnp.bfloat16)


def draw_queries(key, part):
    return beam_draws(key)[2].astype(jnp.bfloat16)


def shard_levels(own_key, shape, pieces, low, top_value):
    def one(position, parts):
        steps = jax.random.uniform(jax.random.fold_in(jax.random.fold_in(own_key, 6), position), (parts,), jnp.float32, low / len(pieces), top_value / len(pieces))
        return jnp.repeat(jnp.exp(steps), shape[position] // parts).reshape((-1,) + (1,) * (len(shape) - position - 1))

    loudness = one(*pieces[0])
    for cut in pieces[1:]:
        loudness = loudness * one(*cut)
    return loudness


def deal_out(own_key, own, number, rows, amount, top, most, skew):
    ranking = jax.random.permutation(own_key, amount)
    packed, usual = portions_of(amount, rows * top, most, skew, True), portions_of(amount, rows * top, most, skew, False)
    places = jnp.arange(amount)

    def named(tallies, offset_by):
        used = int((tallies > 0).sum())
        fixed = max(1, used // 4)
        shifted = fixed + (places - fixed + offset_by * (used - fixed)) % max(1, amount - fixed)
        return jnp.zeros((amount,), jnp.int32).at[ranking[jnp.where(places < fixed, places, shifted)]].set(jnp.asarray(tallies, jnp.int32))

    tallies = jnp.where(number % 4 == 0, named(packed, number // 4), named(usual, number - number // 4 - 1))
    mixed = jax.random.permutation(jax.random.fold_in(own, 3), amount)
    giver, taker = mixed[0:amount // 2 * 2:2], mixed[1:amount // 2 * 2:2]
    margin = jnp.minimum(tallies[giver] - 1, most - tallies[taker]) // 2
    margin = jnp.where((giver == ranking[0]) | (taker == ranking[0]) | (tallies[taker] == 0), 0, jnp.maximum(margin, 0))
    shifted = jax.random.randint(jax.random.fold_in(own, 4), (amount // 2,), 0, 1 << 20) % (margin + 1)
    tallies = tallies.at[giver].add(-shifted).at[taker].add(shifted)
    labels = jnp.searchsorted(jnp.cumsum(tallies), jnp.arange(rows * top), side="right").astype(jnp.int32)
    table = labels.reshape(top, rows).T
    table = table[jax.random.permutation(jax.random.fold_in(own, 1), rows)]
    offset_by = jax.random.randint(jax.random.fold_in(own, 2), (rows, 1), 0, top)
    return jnp.take_along_axis(table, (jnp.arange(top)[None, :] + offset_by) % top, axis=1)


def portions_of(amount, total, reach, skew, full):
    weights = [(1 << 20) // math.isqrt(rank ** skew) + 1 for rank in range(1, amount + 1)]
    largest = reach if full else min(reach, max(-(-total // amount), total * weights[0] // sum(weights)))
    least = 1 if total - largest >= amount - 1 else 0
    given, rest = [largest] + [least] * (amount - 1), total - largest - least * (amount - 1)
    while rest > 0:
        candidates = [i for i in range(1, amount) if given[i] < largest] or [i for i in range(1, amount) if given[i] < reach]
        pool, remaining = sum([weights[i] for i in candidates]), rest
        for i in candidates:
            more = min(reach - given[i], max(1, remaining * weights[i] // pool), rest)
            given[i] = given[i] + more
            rest = rest - more
    return np.array(given)


def normal_values(key, shape, scale, most, cuts=(), kind=jnp.bfloat16):
    values = scale * jax.random.normal(key, shape, jnp.float32)
    if cuts:
        values = values * shard_levels(key, shape, cuts, -0.22, 0.18)
    return jnp.clip(values, -most, most).astype(kind)


def setup_inputs(seed: int = 0, part: int = 0) -> dict:
    splits = jax.random.split(jax.random.key(seed), 14)
    part_keys = jax.random.split(jax.random.fold_in(splits[13], part), 14)
    queries = draw_queries(jax.random.fold_in(jax.random.fold_in(splits[13], part), 71), part)
    new_keys = normal_values(part_keys[1], (BEAMS, D), 1.0, 4.0, ((0, 16),))
    new_values = normal_values(part_keys[2], (BEAMS, D), 1.0, 4.0, ((0, 16),))
    resid = normal_values(part_keys[3], (BEAMS, D), 1.0, 5.0, ((0, 16),))
    key_cache = draw_key_cache(jax.random.fold_in(jax.random.fold_in(splits[13], part), 71), part)
    value_cache = normal_values(part_keys[5], (BEAMS, CTX, D), 1.0, 4.0, ((0, 16),))
    parent = draw_parent(jax.random.fold_in(jax.random.fold_in(splits[13], part), 71), part)
    route_ids_keys = jax.random.split(jax.random.fold_in(part_keys[7], 1), BEAMS // B_DEV)
    route_ids_turns = jax.random.permutation(jax.random.fold_in(part_keys[7], 3), BEAMS // B_DEV)
    route_ids = jax.vmap(lambda own, number: deal_out(jax.random.fold_in(part_keys[7], 2), own, number, B_DEV, EXPERTS, TOPK, CAP, 2))(route_ids_keys, route_ids_turns).reshape((BEAMS, TOPK))
    route_weights = jnp.clip(jax.random.uniform(part_keys[8], (BEAMS, TOPK), jnp.float32, 0.05, 0.35), 0.05, 0.35)
    norm_gain = jnp.clip(1.0 + 0.18 * jax.random.normal(splits[9], (D,), jnp.float32), 0.1, 1.9)
    w_gate = normal_values(splits[10], (EXPERTS, D, FF), D ** -0.5, 0.125, ((0, 16),))
    w_up = normal_values(splits[11], (EXPERTS, D, FF), D ** -0.5, 0.125, ((0, 16),))
    w_down = normal_values(splits[12], (EXPERTS, FF, D), FF ** -0.5, 0.15625, ((0, 16),))
    return dict(queries=queries, new_keys=new_keys, new_values=new_values, resid=resid, key_cache=key_cache, value_cache=value_cache, parent=parent, route_ids=route_ids, route_weights=route_weights, norm_gain=norm_gain, w_gate=w_gate, w_up=w_up, w_down=w_down)


def attend(query_rows, new_key_rows, new_value_rows, key_cache, value_cache):
    slots = query_rows.shape[0]
    scale = 1.0 / math.sqrt(HEAD_DIM)
    query_heads = query_rows.reshape(slots, HEADS, HEAD_DIM).astype(jnp.float32)
    new_key_heads = new_key_rows.reshape(slots, HEADS, HEAD_DIM).astype(jnp.float32)
    new_value_heads = new_value_rows.reshape(slots, HEADS, HEAD_DIM).astype(jnp.float32)
    key_heads = key_cache.reshape(slots, CTX, HEADS, HEAD_DIM).astype(jnp.float32)
    value_heads = value_cache.reshape(slots, CTX, HEADS, HEAD_DIM).astype(jnp.float32)
    scores = jnp.einsum('bhd,bthd->bht', query_heads, key_heads) * scale
    self_score = lax.optimization_barrier(jnp.sum(query_heads * new_key_heads, axis=-1)) * scale
    peak = jnp.maximum(lax.optimization_barrier(jnp.max(scores, axis=-1)), self_score)
    expo = jnp.exp(scores - peak[:, :, None])
    self_expo = jnp.exp(self_score - peak)
    denominator = lax.optimization_barrier(jnp.sum(expo, axis=-1)) + self_expo
    probs_bf = expo.astype(jnp.bfloat16).astype(jnp.float32)
    self_bf = self_expo.astype(jnp.bfloat16).astype(jnp.float32)
    mixed = jnp.einsum('bht,bthd->bhd', probs_bf, value_heads) + self_bf[:, :, None] * new_value_heads
    return (mixed / denominator[:, :, None]).reshape(slots, HEADS * HEAD_DIM).astype(jnp.bfloat16)

def reference(queries, new_keys, new_values, resid, key_cache, value_cache, parent, route_ids, route_weights, norm_gain, w_gate, w_up, w_down):
    order = jnp.arange(BEAMS, dtype=jnp.int32)
    children = jnp.zeros((BEAMS,), jnp.int32).at[parent].set(order)
    attended = attend(queries[children], new_keys[children], new_values[children], key_cache, value_cache)
    hidden_state = resid[children].astype(jnp.float32) + attended.astype(jnp.float32)
    normed = (hidden_state * lax.rsqrt(lax.optimization_barrier(jnp.mean(hidden_state * hidden_state, axis=-1, keepdims=True)) + 1e-06) * norm_gain).astype(jnp.bfloat16)
    expert_ids = jnp.arange(EXPERTS, dtype=jnp.int32)
    coef = lax.optimization_barrier(jnp.sum(route_weights[:, :, None] * (route_ids[:, :, None] == expert_ids[None, None, :]), axis=1))

    def one_expert(totals, index):
        gate_act = jnp.dot(normed, w_gate[index], preferred_element_type=jnp.float32)
        up_act = jnp.dot(normed, w_up[index], preferred_element_type=jnp.float32)
        inner = (jax.nn.silu(gate_act) * up_act).astype(jnp.bfloat16)
        expert_out = jnp.dot(inner, w_down[index], preferred_element_type=jnp.float32)
        weight_col = lax.dynamic_index_in_dim(coef, index, 1, keepdims=True)
        return (totals + weight_col * expert_out, None)
    totals, unused = lax.scan(one_expert, jnp.zeros((BEAMS, HEADS * HEAD_DIM), jnp.float32), expert_ids)
    return (hidden_state + totals).astype(jnp.bfloat16)
```

```python
import functools
import math

import jax
import jax.numpy as jnp
from jax import lax
from jax.experimental import pallas as pl
from jax.experimental.pallas import tpu as pltpu
from jax.sharding import PartitionSpec as P

HEAD_DIM = 128
LANES = 128
PIECES = 4
F32 = jnp.float32
BF16 = jnp.bfloat16


def flip(index, bit):
    return index + bit * (1 - 2 * lax.rem(lax.div(index, bit), 2))


def layer_kernel(
    cfg,
    parent,
    route_ids,
    route_weights,
    gain,
    queries,
    new_keys,
    new_values,
    resid,
    key_cache,
    value_cache,
    w_gate,
    w_up,
    w_down,
    out,
    all_q,
    all_s,
    all_vr,
    own_key,
    keys,
    values,
    gate,
    up,
    down,
    mixed_ref,
    hidden_ref,
    spread,
    disp,
    arrived,
    tokens,
    gate_acc,
    up_acc,
    piece_ref,
    outgoing,
    returned,
    own_sem,
    key_sem,
    value_sem,
    weight_sem,
    send_sem,
    q_sem,
    s_sem,
    vr_sem,
    token_sem,
    back_sem,
):
    experts, beams, minor, capacity = cfg
    count = experts * beams
    major = count // minor
    rows, width = hidden_ref.shape
    heads = width // HEAD_DIM
    chosen = route_ids.shape[1]
    scale = 1.0 / math.sqrt(HEAD_DIM)
    me = lax.axis_index("expert") * beams + lax.axis_index("beam")
    high, low = lax.div(me, minor), lax.rem(me, minor)

    def place(index):
        return {"expert": lax.div(index, beams), "beam": lax.rem(index, beams)}

    def other(step):
        return lax.rem(me + step, count)

    own_copies = [
        pltpu.make_async_copy(queries, all_q.at[me], own_sem.at[0]),
        pltpu.make_async_copy(new_keys, own_key, own_sem.at[1]),
        pltpu.make_async_copy(new_values, all_vr.at[me, 0], own_sem.at[2]),
        pltpu.make_async_copy(resid, all_vr.at[me, 1], own_sem.at[3]),
    ]
    for copy in own_copies:
        copy.start()
    barrier = pltpu.get_barrier_semaphore()
    for step in range(1, count):
        pl.semaphore_signal(
            barrier,
            inc=1,
            device_id=place(other(step)),
            device_id_type=pl.DeviceIdType.MESH,
        )
    key_copies = []
    value_copies = []
    for slot in range(rows):
        key_copies.append(
            pltpu.make_async_copy(key_cache.at[slot], keys.at[slot], key_sem.at[slot])
        )
    for slot in range(rows):
        value_copies.append(
            pltpu.make_async_copy(value_cache.at[slot], values.at[slot], value_sem.at[slot])
        )
    for copy in key_copies + value_copies:
        copy.start()
    weight_waits = []
    for number, (source, target) in enumerate(((w_gate, gate), (w_up, up), (w_down, down))):
        depth = target.shape[0]
        part = depth // 4
        for chunk in range(4):
            span = pl.ds(chunk * part, part)
            pltpu.make_async_copy(
                source.at[0, span, :], target.at[span, :], weight_sem.at[number]
            ).start()
        weight_waits.append(pltpu.make_async_copy(target, target, weight_sem.at[number]))

    def push(buffer, block, target, send, receive):
        pltpu.make_async_remote_copy(
            src_ref=buffer.at[block],
            dst_ref=buffer.at[block],
            send_sem=send,
            recv_sem=receive.at[block],
            device_id=place(target),
            device_id_type=pl.DeviceIdType.MESH,
        ).start()

    def landed(buffer, block, receive):
        pltpu.make_async_copy(buffer.at[block], buffer.at[block], receive.at[block]).wait()

    bits = []
    bit = minor // 2
    while bit >= 1:
        bits.append(bit)
        bit //= 2


    def block_of(step, flips):
        lane = low
        for b in flips:
            lane = flip(lane, b)
        return lax.rem(high + step, major) * minor + lane

    def subsets(names):
        found = [()]
        for b in names:
            found = found + [f + (b,) for f in found]
        return found

    def push_own(buffer, send, receive):
        for step in range(1, major):
            push(buffer, me, block_of(step, ()), send, receive)
        for b in bits:
            push(buffer, me, flip(me, b), send, receive)

    def forward_line(buffer, send, receive):
        for step in range(1, major):
            block = block_of(step, ())
            landed(buffer, block, receive)
            for b in bits:
                push(buffer, block, flip(me, b), send, receive)

    def forward_level(buffer, level, send, receive):
        for flips in subsets(bits[:level]):
            for step in range(major):
                block = block_of(step, flips + (bits[level],))
                landed(buffer, block, receive)
                for b in bits[level + 1 :]:
                    push(buffer, block, flip(me, b), send, receive)

    first_slot = me * rows

    def find_child(beam, found):
        origin = parent[beam]
        return tuple(
            jnp.where(origin == first_slot + slot, beam, found[slot]) for slot in range(rows)
        )

    own_copies[0].wait()
    own_copies[1].wait()
    product = all_q[me].astype(F32) * own_key[...].astype(F32)
    lane = lax.broadcasted_iota(jnp.int32, (rows, LANES), 1)
    self_rows = jnp.zeros((rows, LANES), F32)
    for head in range(heads):
        total = jnp.sum(
            product[:, head * HEAD_DIM : (head + 1) * HEAD_DIM], axis=1, keepdims=True
        )
        self_rows = jnp.where(lane == head, total * scale, self_rows)
    all_s[me] = self_rows
    own_copies[2].wait()
    own_copies[3].wait()

    pl.semaphore_wait(barrier, count - 1)
    push_own(all_q, send_sem.at[0], q_sem)
    push_own(all_s, send_sem.at[1], s_sem)
    push_own(all_vr, send_sem.at[2], vr_sem)
    child = lax.fori_loop(
        0, parent.shape[0], find_child, tuple(jnp.int32(0) for _ in range(rows))
    )

    places = experts * capacity

    def slot_tables(shape, dimension):
        numbers = lax.broadcasted_iota(jnp.int32, shape, dimension)
        expert_of, rank_of = lax.div(numbers, capacity), lax.rem(numbers, capacity)
        ranks = jnp.zeros(shape, jnp.int32)
        placed, weights = [], []
        for slot in range(rows):
            named = jnp.zeros(shape, jnp.int32)
            weight = jnp.zeros(shape, F32)
            for pick in range(chosen):
                hit = expert_of == route_ids[first_slot + slot, pick]
                named = jnp.where(hit, 1, named)
                weight = weight + jnp.where(hit, route_weights[first_slot + slot, pick], 0.0)
            mine = (named == 1) & (ranks == rank_of)
            placed.append(jnp.where(mine, 1.0, 0.0))
            weights.append(jnp.where(mine, weight, 0.0))
            ranks = ranks + named
        return placed, weights

    placed, _ = slot_tables((places, 1), 0)
    lanes_of_places = -(-places // LANES) * LANES
    _, lane_weights = slot_tables((1, lanes_of_places), 1)
    row_number = lax.broadcasted_iota(jnp.int32, (rows, lanes_of_places), 0)
    combine = jnp.zeros((rows, lanes_of_places), F32)
    for slot in range(rows):
        combine = jnp.where(row_number == slot, lane_weights[slot], combine)

    forward_line(all_q, send_sem.at[0], q_sem)
    forward_line(all_s, send_sem.at[1], s_sem)
    levels = len(bits)
    for level in range(levels):
        forward_level(all_q, level, send_sem.at[0], q_sem)
        forward_level(all_s, level, send_sem.at[1], s_sem)
        if level == 0:
            forward_line(all_vr, send_sem.at[2], vr_sem)

    head_mask = lax.broadcasted_iota(jnp.int32, (heads, width), 0) == lax.div(
        lax.broadcasted_iota(jnp.int32, (heads, width), 1), HEAD_DIM
    )
    self_mask = lax.broadcasted_iota(jnp.int32, (heads, LANES), 0) == lax.broadcasted_iota(
        jnp.int32, (heads, LANES), 1
    )

    def pick(block, row):
        block = block.astype(F32)
        chosen_row = lax.broadcasted_iota(jnp.int32, block.shape, 0) == row
        return jnp.sum(jnp.where(chosen_row, block, 0.0), axis=0, keepdims=True)

    probs, selfs, denominators = [], [], []
    for slot in range(rows):
        device, row = lax.div(child[slot], rows), lax.rem(child[slot], rows)
        query = pick(all_q[device], row)
        spread_query = jnp.where(head_mask, query, 0.0).astype(BF16)
        key_copies[slot].wait()
        scores = (
            lax.dot_general(
                spread_query,
                keys[slot],
                (((1,), (1,)), ((), ())),
                preferred_element_type=F32,
            )
            * scale
        )
        self_score = jnp.sum(
            jnp.where(self_mask, pick(all_s[device], row), 0.0), axis=1, keepdims=True
        )
        peak = jnp.maximum(jnp.max(scores, axis=1, keepdims=True), self_score)
        expo = jnp.exp(scores - peak)
        self_expo = jnp.exp(self_score - peak)
        denominators.append(jnp.sum(expo, axis=1, keepdims=True) + self_expo)
        probs.append(expo.astype(BF16))
        selfs.append(self_expo.astype(BF16).astype(F32))
    for slot in range(rows):
        value_copies[slot].wait()
        mixed_ref[slot] = jnp.dot(probs[slot], values[slot], preferred_element_type=F32)
    for level in range(levels):
        forward_level(all_vr, level, send_sem.at[2], vr_sem)

    gains = gain[...]
    normed = []
    for slot in range(rows):
        device, row = lax.div(child[slot], rows), lax.rem(child[slot], rows)
        new_value = pick(all_vr[device, 0], row)
        residual = pick(all_vr[device, 1], row)
        mixed = (mixed_ref[slot] + selfs[slot] * new_value) / denominators[slot]
        attended = jnp.sum(jnp.where(head_mask, mixed, 0.0), axis=0, keepdims=True)
        hidden = residual + attended.astype(BF16).astype(F32)
        hidden_ref[pl.ds(slot, 1), :] = hidden
        mean = jnp.mean(hidden * hidden, axis=1, keepdims=True)
        row_normed = (hidden * lax.rsqrt(mean + 1e-06) * gains).astype(BF16)
        normed.append(row_normed.astype(F32))
    total = placed[0] * normed[0]
    for slot in range(1, rows):
        total = total + placed[slot] * normed[slot]
    spread[...] = total
    for expert in range(experts):
        disp[expert] = spread[pl.ds(expert * capacity, capacity), :].astype(BF16)
    for step in range(1, count):
        target = other(step)
        pltpu.make_async_remote_copy(
            src_ref=disp.at[lax.div(target, beams)],
            dst_ref=arrived.at[me],
            send_sem=send_sem.at[3],
            recv_sem=token_sem.at[me],
            device_id=place(target),
            device_id_type=pl.DeviceIdType.MESH,
        ).start()
    arrived[me] = disp[lax.div(me, beams)]
    for source in range(count):

        @pl.when(me != source)
        def _():
            landed(arrived, source, token_sem)

        tokens[pl.ds(source * capacity, capacity), :] = arrived[source].astype(F32)

    weight_waits[0].wait()
    weight_waits[1].wait()
    chunk = 256 if width % 256 == 0 else LANES
    gate_acc[...] = jnp.zeros_like(gate_acc)
    up_acc[...] = jnp.zeros_like(up_acc)

    def gate_up(step, carry):
        span = pl.ds(pl.multiple_of(step * chunk, chunk), chunk)
        left = tokens[:, span].astype(BF16)
        gate_acc[...] += jnp.dot(left, gate[span, :], preferred_element_type=F32)
        up_acc[...] += jnp.dot(left, up[span, :], preferred_element_type=F32)
        return carry

    lax.fori_loop(0, width // chunk, gate_up, 0)
    activation = gate_acc[...]
    inner = (activation / (1.0 + jnp.exp(-activation)) * up_acc[...]).astype(BF16)
    weight_waits[2].wait()
    part = width // PIECES
    for piece in range(PIECES):
        piece_ref[...] = jnp.dot(
            inner, down[:, piece * part : (piece + 1) * part], preferred_element_type=F32
        )
        for source in range(count):
            outgoing[piece, source] = piece_ref[pl.ds(source * capacity, capacity), :].astype(BF16)
        for step in range(1, count):
            target = other(step)
            pltpu.make_async_remote_copy(
                src_ref=outgoing.at[piece, target],
                dst_ref=returned.at[piece, me],
                send_sem=send_sem.at[4 + piece],
                recv_sem=back_sem.at[piece],
                device_id=place(target),
                device_id_type=pl.DeviceIdType.MESH,
            ).start()
        returned[piece, me] = outgoing[piece, me]

    for piece in range(PIECES):
        rest = returned.at[piece, pl.ds(0, count - 1)]
        pltpu.make_async_copy(rest, rest, back_sem.at[piece]).wait()
        columns = pl.ds(piece * part, part)
        sums = hidden_ref[:, columns]
        for source in range(count):
            block = returned[piece, source].astype(F32)
            for rank in range(capacity):
                at = (source // beams) * capacity + rank
                sums = sums + combine[:, at : at + 1] * block[rank : rank + 1, :]
        out[:, columns] = sums.astype(out.dtype)

    for number, buffer in enumerate((all_q, all_s, all_vr, arrived)):
        sent = buffer.at[pl.ds(0, count - 1)]
        pltpu.make_async_copy(sent, sent, send_sem.at[number]).wait()
    for piece in range(PIECES):
        sent = outgoing.at[piece, pl.ds(0, count - 1)]
        pltpu.make_async_copy(sent, sent, send_sem.at[4 + piece]).wait()


def body(
    queries,
    new_keys,
    new_values,
    resid,
    key_cache,
    value_cache,
    parent,
    route_ids,
    route_weights,
    norm_gain,
    w_gate,
    w_up,
    w_down,
):
    rows, width = queries.shape
    positions = key_cache.shape[1]
    hidden_units = w_gate.shape[2]
    experts, beams = lax.axis_size("expert"), lax.axis_size("beam")
    count = experts * beams
    minor = beams
    while minor < 4 and beams == 1 and experts % (2 * minor) == 0:
        minor *= 2
    capacity = max(2, -(-rows * route_ids.shape[1] // experts))
    heads = width // HEAD_DIM
    part = width // PIECES
    vmem = pltpu.VMEM
    smem_spec = pl.BlockSpec(memory_space=pltpu.SMEM)
    any_spec = pl.BlockSpec(memory_space=pl.ANY)
    vmem_spec = pl.BlockSpec(memory_space=pltpu.VMEM)
    dma = pltpu.SemaphoreType.DMA
    return pl.pallas_call(
        functools.partial(layer_kernel, (experts, beams, minor, capacity)),
        out_shape=jax.ShapeDtypeStruct((rows, width), BF16),
        in_specs=[smem_spec] * 3 + [vmem_spec] + [any_spec] * 9,
        out_specs=vmem_spec,
        scratch_shapes=[
            vmem((count, rows, width), BF16),
            vmem((count, rows, LANES), F32),
            vmem((count, 2, rows, width), BF16),
            vmem((rows, width), BF16),
            vmem((rows, positions, width), BF16),
            vmem((rows, positions, width), BF16),
            vmem((width, hidden_units), BF16),
            vmem((width, hidden_units), BF16),
            vmem((hidden_units, width), BF16),
            vmem((rows, heads, width), F32),
            vmem((rows, width), F32),
            vmem((experts * capacity, width), F32),
            vmem((experts, capacity, width), BF16),
            vmem((count, capacity, width), BF16),
            vmem((count * capacity, width), F32),
            vmem((count * capacity, hidden_units), F32),
            vmem((count * capacity, hidden_units), F32),
            vmem((count * capacity, part), F32),
            vmem((PIECES, count, capacity, part), BF16),
            vmem((PIECES, count, capacity, part), BF16),
            dma((4,)),
            dma((rows,)),
            dma((rows,)),
            dma((3,)),
            dma((4 + PIECES,)),
            dma((count,)),
            dma((count,)),
            dma((count,)),
            dma((count,)),
            dma((PIECES,)),
        ],
        compiler_params=pltpu.CompilerParams(collective_id=0, has_side_effects=True),
    )(
        parent,
        route_ids,
        route_weights,
        norm_gain[None, :],
        queries,
        new_keys,
        new_values,
        resid,
        key_cache,
        value_cache,
        w_gate,
        w_up,
        w_down,
    )


def solution(mesh):
    return jax.shard_map(
        body,
        mesh=mesh,
        in_specs=(
            P(("groups", "expert", "beam"), None),
            P(("groups", "expert", "beam"), None),
            P(("groups", "expert", "beam"), None),
            P(("groups", "expert", "beam"), None),
            P(("groups", "expert", "beam"), None, None),
            P(("groups", "expert", "beam"), None, None),
            P("groups"),
            P("groups", None),
            P("groups", None),
            P(),
            P("expert", None, "beam"),
            P("expert", None, "beam"),
            P("expert", "beam", None),
        ),
        out_specs=P(("groups", "expert", "beam"), None),
        check_vma=False,
    )
```

```python
import functools
import math

import jax
import jax.numpy as jnp
from jax import lax
from jax.experimental import pallas as pl
from jax.experimental.pallas import tpu as pltpu
from jax.sharding import PartitionSpec as P

HEAD_DIM = 128
LANES = 128
PIECES = 4
F32 = jnp.float32
BF16 = jnp.bfloat16


def flip(index, bit):
    return index + bit * (1 - 2 * lax.rem(lax.div(index, bit), 2))


def layer_kernel(
    cfg,
    parent_in,
    route_ids_in,
    route_weights_in,
    gain_in,
    queries,
    new_keys,
    new_values,
    resid,
    key_cache,
    value_cache,
    w_gate,
    w_up,
    w_down,
    out,
    parent,
    route_ids,
    route_weights,
    gain,
    all_q,
    all_s,
    all_vr,
    own_key,
    keys,
    values,
    gate,
    up,
    down,
    mixed_ref,
    hidden_ref,
    spread,
    disp,
    arrived,
    tokens,
    gate_acc,
    up_acc,
    piece_ref,
    outgoing,
    returned,
    own_sem,
    key_sem,
    value_sem,
    weight_sem,
    send_sem,
    q_sem,
    s_sem,
    vr_sem,
    token_sem,
    back_sem,
):
    experts, beams, minor, capacity = cfg
    count = experts * beams
    major = count // minor
    rows, width = hidden_ref.shape
    heads = width // HEAD_DIM
    chosen = route_ids.shape[0]
    scale = 1.0 / math.sqrt(HEAD_DIM)
    me = lax.axis_index("expert") * beams + lax.axis_index("beam")
    high, low = lax.div(me, minor), lax.rem(me, minor)

    def place(index):
        return {"expert": lax.div(index, beams), "beam": lax.rem(index, beams)}

    def other(step):
        return lax.rem(me + step, count)

    own_copies = [
        pltpu.make_async_copy(queries, all_q.at[me], own_sem.at[0]),
        pltpu.make_async_copy(new_keys, own_key, own_sem.at[1]),
        pltpu.make_async_copy(new_values, all_vr.at[me, 0], own_sem.at[2]),
        pltpu.make_async_copy(resid, all_vr.at[me, 1], own_sem.at[3]),
    ]
    small_copies = [
        pltpu.make_async_copy(parent_in, parent, own_sem.at[4]),
        pltpu.make_async_copy(route_ids_in, route_ids, own_sem.at[5]),
        pltpu.make_async_copy(route_weights_in, route_weights, own_sem.at[6]),
        pltpu.make_async_copy(gain_in, gain, own_sem.at[7]),
    ]
    bits = []
    bit = minor // 2
    while bit >= 1:
        bits.append(bit)
        bit //= 2

    def block_of(step, flips):
        lane = low
        for b in flips:
            lane = flip(lane, b)
        return lax.rem(high + step, major) * minor + lane

    barrier = pltpu.get_barrier_semaphore()
    greeted = [block_of(step, ()) for step in range(1, major)] + [flip(me, b) for b in bits]
    for target in greeted:
        pl.semaphore_signal(
            barrier,
            inc=1,
            device_id=place(target),
            device_id_type=pl.DeviceIdType.MESH,
        )
    for copy in own_copies + small_copies:
        copy.start()
    key_copies = []
    value_copies = []
    for slot in range(rows):
        key_copies.append(
            pltpu.make_async_copy(key_cache.at[slot], keys.at[slot], key_sem.at[slot])
        )
    for slot in range(rows):
        value_copies.append(
            pltpu.make_async_copy(value_cache.at[slot], values.at[slot], value_sem.at[slot])
        )
    for copy in key_copies + value_copies:
        copy.start()
    weight_waits = []
    for number, (source, target) in enumerate(((w_gate, gate), (w_up, up), (w_down, down))):
        depth = target.shape[0]
        part = depth // 4
        for chunk in range(4):
            span = pl.ds(chunk * part, part)
            pltpu.make_async_copy(
                source.at[0, span, :], target.at[span, :], weight_sem.at[number]
            ).start()
        weight_waits.append(pltpu.make_async_copy(target, target, weight_sem.at[number]))

    def push(buffer, block, target, send, receive):
        pltpu.make_async_remote_copy(
            src_ref=buffer.at[block],
            dst_ref=buffer.at[block],
            send_sem=send,
            recv_sem=receive.at[block],
            device_id=place(target),
            device_id_type=pl.DeviceIdType.MESH,
        ).start()

    def landed(buffer, block, receive):
        pltpu.make_async_copy(buffer.at[block], buffer.at[block], receive.at[block]).wait()

    def subsets(names):
        found = [()]
        for b in names:
            found = found + [f + (b,) for f in found]
        return found

    def push_own(buffer, send, receive):
        for step in range(1, major):
            push(buffer, me, block_of(step, ()), send, receive)
        for b in bits:
            push(buffer, me, flip(me, b), send, receive)

    def forward_line(buffer, send, receive, steps=None):
        for step in range(1, major) if steps is None else steps:
            block = block_of(step, ())
            landed(buffer, block, receive)
            for b in bits:
                push(buffer, block, flip(me, b), send, receive)

    def forward_level(buffer, level, send, receive, steps=None):
        for flips in subsets(bits[:level]):
            for step in range(major) if steps is None else steps:
                block = block_of(step, flips + (bits[level],))
                landed(buffer, block, receive)
                for b in bits[level + 1 :]:
                    push(buffer, block, flip(me, b), send, receive)

    first_slot = me * rows

    def find_child(beam, found):
        origin = parent[beam]
        return tuple(
            jnp.where(origin == first_slot + slot, beam, found[slot]) for slot in range(rows)
        )

    own_copies[0].wait()
    pl.semaphore_wait(barrier, len(greeted))
    push_own(all_q, send_sem.at[0], q_sem)
    own_copies[1].wait()
    product = all_q[me].astype(F32) * own_key[...].astype(F32)
    lane = lax.broadcasted_iota(jnp.int32, (rows, LANES), 1)
    self_rows = jnp.zeros((rows, LANES), F32)
    for head in range(heads):
        total = jnp.sum(
            product[:, head * HEAD_DIM : (head + 1) * HEAD_DIM], axis=1, keepdims=True
        )
        self_rows = jnp.where(lane == head, total * scale, self_rows)
    all_s[me] = self_rows
    own_copies[2].wait()
    own_copies[3].wait()
    push_own(all_s, send_sem.at[1], s_sem)
    push_own(all_vr, send_sem.at[2], vr_sem)
    for copy in small_copies:
        copy.wait()
    child = lax.fori_loop(
        0, parent.shape[0], find_child, tuple(jnp.int32(0) for _ in range(rows))
    )

    places = experts * capacity

    def slot_tables(shape, dimension):
        numbers = lax.broadcasted_iota(jnp.int32, shape, dimension)
        expert_of, rank_of = lax.div(numbers, capacity), lax.rem(numbers, capacity)
        ranks = jnp.zeros(shape, jnp.int32)
        placed, weights = [], []
        for slot in range(rows):
            named = jnp.zeros(shape, jnp.int32)
            weight = jnp.zeros(shape, F32)
            for pick in range(chosen):
                hit = expert_of == route_ids[pick, first_slot + slot]
                named = jnp.where(hit, 1, named)
                weight = weight + jnp.where(hit, route_weights[pick, first_slot + slot], 0.0)
            mine = (named == 1) & (ranks == rank_of)
            placed.append(jnp.where(mine, 1.0, 0.0))
            weights.append(jnp.where(mine, weight, 0.0))
            ranks = ranks + named
        return placed, weights

    placed, _ = slot_tables((places, 1), 0)
    lanes_of_places = -(-places // LANES) * LANES
    _, lane_weights = slot_tables((1, lanes_of_places), 1)
    row_number = lax.broadcasted_iota(jnp.int32, (rows, lanes_of_places), 0)
    combine = jnp.zeros((rows, lanes_of_places), F32)
    for slot in range(rows):
        combine = jnp.where(row_number == slot, lane_weights[slot], combine)

    forward_line(all_q, send_sem.at[0], q_sem)
    forward_line(all_s, send_sem.at[1], s_sem)
    levels = len(bits)
    for level in range(levels):
        if level == 0:
            for step in range(major):
                forward_level(all_q, level, send_sem.at[0], q_sem, (step,))
                if step > 0:
                    forward_line(all_vr, send_sem.at[2], vr_sem, (step,))
        else:
            forward_level(all_q, level, send_sem.at[0], q_sem)
        forward_level(all_s, level, send_sem.at[1], s_sem)

    head_mask = lax.broadcasted_iota(jnp.int32, (heads, width), 0) == lax.div(
        lax.broadcasted_iota(jnp.int32, (heads, width), 1), HEAD_DIM
    )
    self_mask = lax.broadcasted_iota(jnp.int32, (heads, LANES), 0) == lax.broadcasted_iota(
        jnp.int32, (heads, LANES), 1
    )

    def pick(block, row):
        block = block.astype(F32)
        chosen_row = lax.broadcasted_iota(jnp.int32, block.shape, 0) == row
        return jnp.sum(jnp.where(chosen_row, block, 0.0), axis=0, keepdims=True)

    probs, selfs, denominators = [], [], []
    for slot in range(rows):
        device, row = lax.div(child[slot], rows), lax.rem(child[slot], rows)
        query = pick(all_q[device], row)
        spread_query = jnp.where(head_mask, query, 0.0).astype(BF16)
        key_copies[slot].wait()
        scores = (
            lax.dot_general(
                spread_query,
                keys[slot],
                (((1,), (1,)), ((), ())),
                preferred_element_type=F32,
            )
            * scale
        )
        self_score = jnp.sum(
            jnp.where(self_mask, pick(all_s[device], row), 0.0), axis=1, keepdims=True
        )
        peak = jnp.maximum(jnp.max(scores, axis=1, keepdims=True), self_score)
        expo = jnp.exp(scores - peak)
        self_expo = jnp.exp(self_score - peak)
        denominators.append(jnp.sum(expo, axis=1, keepdims=True) + self_expo)
        probs.append(expo.astype(BF16))
        selfs.append(self_expo.astype(BF16).astype(F32))
    for slot in range(rows):
        value_copies[slot].wait()
        mixed_ref[slot] = jnp.dot(probs[slot], values[slot], preferred_element_type=F32)
    for level in range(levels):
        forward_level(all_vr, level, send_sem.at[2], vr_sem)

    gains = gain[...]
    normed = []
    for slot in range(rows):
        device, row = lax.div(child[slot], rows), lax.rem(child[slot], rows)
        new_value = pick(all_vr[device, 0], row)
        residual = pick(all_vr[device, 1], row)
        mixed = (mixed_ref[slot] + selfs[slot] * new_value) / denominators[slot]
        attended = jnp.sum(jnp.where(head_mask, mixed, 0.0), axis=0, keepdims=True)
        hidden = residual + attended.astype(BF16).astype(F32)
        hidden_ref[pl.ds(slot, 1), :] = hidden
        mean = jnp.mean(hidden * hidden, axis=1, keepdims=True)
        row_normed = (hidden * lax.rsqrt(mean + 1e-06) * gains).astype(BF16)
        normed.append(row_normed.astype(F32))
    total = placed[0] * normed[0]
    for slot in range(1, rows):
        total = total + placed[slot] * normed[slot]
    spread[...] = total
    part = width // PIECES
    for piece in range(PIECES):
        columns = pl.ds(piece * part, part)
        for expert in range(experts):
            disp[piece, expert] = spread[pl.ds(expert * capacity, capacity), columns].astype(BF16)
        for step in range(1, count):
            target = other(step)
            pltpu.make_async_remote_copy(
                src_ref=disp.at[piece, lax.div(target, beams)],
                dst_ref=arrived.at[piece, me],
                send_sem=send_sem.at[3 + piece],
                recv_sem=token_sem.at[piece],
                device_id=place(target),
                device_id_type=pl.DeviceIdType.MESH,
            ).start()
        arrived[piece, me] = disp[piece, lax.div(me, beams)]

    def rest_of(buffer, piece):
        return buffer.at[piece, pl.ds(0, count - 1)]

    for piece in range(PIECES):
        rest = rest_of(arrived, piece)
        pltpu.make_async_copy(rest, rest, token_sem.at[piece]).wait()
        for source in range(count):
            tokens[pl.ds(source * capacity, capacity), :] = arrived[piece, source].astype(F32)
        if piece == 0:
            weight_waits[0].wait()
            weight_waits[1].wait()
        span = pl.ds(piece * part, part)
        left = tokens[...].astype(BF16)
        gate_part = jnp.dot(left, gate[span, :], preferred_element_type=F32)
        up_part = jnp.dot(left, up[span, :], preferred_element_type=F32)
        if piece == 0:
            gate_acc[...] = gate_part
            up_acc[...] = up_part
        else:
            gate_acc[...] += gate_part
            up_acc[...] += up_part
    activation = gate_acc[...]
    inner = (activation / (1.0 + jnp.exp(-activation)) * up_acc[...]).astype(BF16)
    weight_waits[2].wait()
    for piece in range(PIECES):
        piece_ref[...] = jnp.dot(
            inner, down[:, piece * part : (piece + 1) * part], preferred_element_type=F32
        )
        for source in range(count):
            outgoing[piece, source] = piece_ref[pl.ds(source * capacity, capacity), :].astype(BF16)
        for step in range(1, count):
            target = other(step)
            pltpu.make_async_remote_copy(
                src_ref=outgoing.at[piece, target],
                dst_ref=returned.at[piece, me],
                send_sem=send_sem.at[3 + PIECES + piece],
                recv_sem=back_sem.at[piece],
                device_id=place(target),
                device_id_type=pl.DeviceIdType.MESH,
            ).start()
        returned[piece, me] = outgoing[piece, me]

    for piece in range(PIECES):
        rest = rest_of(returned, piece)
        pltpu.make_async_copy(rest, rest, back_sem.at[piece]).wait()
        columns = pl.ds(piece * part, part)
        sums = hidden_ref[:, columns]
        for source in range(count):
            block = returned[piece, source].astype(F32)
            for rank in range(capacity):
                at = (source // beams) * capacity + rank
                sums = sums + combine[:, at : at + 1] * block[rank : rank + 1, :]
        out[:, columns] = sums.astype(out.dtype)

    for number, buffer in enumerate((all_q, all_s, all_vr)):
        sent = buffer.at[pl.ds(0, count - 1)]
        pltpu.make_async_copy(sent, sent, send_sem.at[number]).wait()
    for piece in range(PIECES):
        for number, buffer in ((3, arrived), (3 + PIECES, outgoing)):
            sent = rest_of(buffer, piece)
            pltpu.make_async_copy(sent, sent, send_sem.at[number + piece]).wait()


def body(
    queries,
    new_keys,
    new_values,
    resid,
    key_cache,
    value_cache,
    parent,
    route_ids,
    route_weights,
    norm_gain,
    w_gate,
    w_up,
    w_down,
):
    rows, width = queries.shape
    positions = key_cache.shape[1]
    hidden_units = w_gate.shape[2]
    experts, beams = lax.axis_size("expert"), lax.axis_size("beam")
    count = experts * beams
    minor = beams
    while minor < 4 and beams == 1 and experts % (2 * minor) == 0:
        minor *= 2
    capacity = max(2, -(-rows * route_ids.shape[1] // experts))
    heads = width // HEAD_DIM
    part = width // PIECES
    vmem = pltpu.VMEM
    smem = pltpu.SMEM
    any_spec = pl.BlockSpec(memory_space=pl.ANY)
    vmem_spec = pl.BlockSpec(memory_space=pltpu.VMEM)
    dma = pltpu.SemaphoreType.DMA
    return pl.pallas_call(
        functools.partial(layer_kernel, (experts, beams, minor, capacity)),
        out_shape=jax.ShapeDtypeStruct((rows, width), BF16),
        in_specs=[any_spec] * 13,
        out_specs=vmem_spec,
        scratch_shapes=[
            smem(parent.shape, jnp.int32),
            smem(route_ids.shape[::-1], jnp.int32),
            smem(route_weights.shape[::-1], F32),
            vmem((1, width), F32),
            vmem((count, rows, width), BF16),
            vmem((count, rows, LANES), F32),
            vmem((count, 2, rows, width), BF16),
            vmem((rows, width), BF16),
            vmem((rows, positions, width), BF16),
            vmem((rows, positions, width), BF16),
            vmem((width, hidden_units), BF16),
            vmem((width, hidden_units), BF16),
            vmem((hidden_units, width), BF16),
            vmem((rows, heads, width), F32),
            vmem((rows, width), F32),
            vmem((experts * capacity, width), F32),
            vmem((PIECES, experts, capacity, part), BF16),
            vmem((PIECES, count, capacity, part), BF16),
            vmem((count * capacity, part), F32),
            vmem((count * capacity, hidden_units), F32),
            vmem((count * capacity, hidden_units), F32),
            vmem((count * capacity, part), F32),
            vmem((PIECES, count, capacity, part), BF16),
            vmem((PIECES, count, capacity, part), BF16),
            dma((8,)),
            dma((rows,)),
            dma((rows,)),
            dma((3,)),
            dma((3 + 2 * PIECES,)),
            dma((count,)),
            dma((count,)),
            dma((count,)),
            dma((PIECES,)),
            dma((PIECES,)),
        ],
        compiler_params=pltpu.CompilerParams(collective_id=0, has_side_effects=True),
    )(
        parent,
        route_ids.T,
        route_weights.T,
        norm_gain[None, :],
        queries,
        new_keys,
        new_values,
        resid,
        key_cache,
        value_cache,
        w_gate,
        w_up,
        w_down,
    )


def solution(mesh):
    return jax.shard_map(
        body,
        mesh=mesh,
        in_specs=(
            P(("groups", "expert", "beam"), None),
            P(("groups", "expert", "beam"), None),
            P(("groups", "expert", "beam"), None),
            P(("groups", "expert", "beam"), None),
            P(("groups", "expert", "beam"), None, None),
            P(("groups", "expert", "beam"), None, None),
            P("groups"),
            P("groups", None),
            P("groups", None),
            P(),
            P("expert", None, "beam"),
            P("expert", None, "beam"),
            P("expert", "beam", None),
        ),
        out_specs=P(("groups", "expert", "beam"), None),
        check_vma=False,
    )
```

```python
import functools
import math

import jax
import jax.numpy as jnp
from jax import lax
from jax.experimental import pallas as pl
from jax.experimental.pallas import tpu as pltpu
from jax.sharding import PartitionSpec as P

HEAD_DIM = 128
LANES = 128
PIECES = 4
F32 = jnp.float32
BF16 = jnp.bfloat16


def flip(index, bit):
    return index + bit * (1 - 2 * lax.rem(lax.div(index, bit), 2))


def layer_kernel(
    cfg,
    parent_in,
    route_ids_in,
    route_weights_in,
    gain_in,
    queries,
    new_keys,
    new_values,
    resid,
    key_cache,
    value_cache,
    w_gate,
    w_up,
    w_down,
    out,
    parent,
    route_ids,
    route_weights,
    gain,
    all_q,
    all_s,
    all_vr,
    own_key,
    keys,
    values,
    gate,
    up,
    down,
    mixed_ref,
    hidden_ref,
    spread,
    disp,
    arrived,
    tokens,
    gate_acc,
    up_acc,
    piece_ref,
    outgoing,
    returned,
    own_sem,
    key_sem,
    value_sem,
    weight_sem,
    send_sem,
    q_sem,
    s_sem,
    vr_sem,
    token_sem,
    back_sem,
):
    experts, beams, minor, capacity = cfg
    count = experts * beams
    major = count // minor
    rows, width = hidden_ref.shape
    heads = width // HEAD_DIM
    chosen = route_ids.shape[0]
    scale = 1.0 / math.sqrt(HEAD_DIM)
    me = lax.axis_index("expert") * beams + lax.axis_index("beam")
    high, low = lax.div(me, minor), lax.rem(me, minor)

    def place(index):
        return {"expert": lax.div(index, beams), "beam": lax.rem(index, beams)}

    def other(step):
        return lax.rem(me + step, count)

    own_copies = [
        pltpu.make_async_copy(queries, all_q.at[me], own_sem.at[0]),
        pltpu.make_async_copy(new_keys, own_key, own_sem.at[1]),
        pltpu.make_async_copy(new_values, all_vr.at[me, 0], own_sem.at[2]),
        pltpu.make_async_copy(resid, all_vr.at[me, 1], own_sem.at[3]),
    ]
    small_copies = [
        pltpu.make_async_copy(parent_in, parent, own_sem.at[4]),
        pltpu.make_async_copy(route_ids_in, route_ids, own_sem.at[5]),
        pltpu.make_async_copy(route_weights_in, route_weights, own_sem.at[6]),
        pltpu.make_async_copy(gain_in, gain, own_sem.at[7]),
    ]
    bits = []
    bit = minor // 2
    while bit >= 1:
        bits.append(bit)
        bit //= 2

    def block_of(step, flips):
        lane = low
        for b in flips:
            lane = flip(lane, b)
        return lax.rem(high + step, major) * minor + lane

    barrier = pltpu.get_barrier_semaphore()
    greeted = [block_of(step, ()) for step in range(1, major)] + [flip(me, b) for b in bits]
    for target in greeted:
        pl.semaphore_signal(
            barrier,
            inc=1,
            device_id=place(target),
            device_id_type=pl.DeviceIdType.MESH,
        )
    for copy in own_copies + small_copies:
        copy.start()
    key_copies = []
    value_copies = []
    for slot in range(rows):
        key_copies.append(
            pltpu.make_async_copy(key_cache.at[slot], keys.at[slot], key_sem.at[slot])
        )
    for slot in range(rows):
        value_copies.append(
            pltpu.make_async_copy(value_cache.at[slot], values.at[slot], value_sem.at[slot])
        )
    for copy in key_copies + value_copies:
        copy.start()
    def push(buffer, block, target, send, receive):
        pltpu.make_async_remote_copy(
            src_ref=buffer.at[block],
            dst_ref=buffer.at[block],
            send_sem=send,
            recv_sem=receive.at[block],
            device_id=place(target),
            device_id_type=pl.DeviceIdType.MESH,
        ).start()

    def landed(buffer, block, receive):
        pltpu.make_async_copy(buffer.at[block], buffer.at[block], receive.at[block]).wait()

    def subsets(names):
        found = [()]
        for b in names:
            found = found + [f + (b,) for f in found]
        return found

    def push_own(buffer, send, receive):
        for step in range(1, major):
            push(buffer, me, block_of(step, ()), send, receive)
        for b in bits:
            push(buffer, me, flip(me, b), send, receive)

    def forward_line(buffer, send, receive, steps=None):
        for step in range(1, major) if steps is None else steps:
            block = block_of(step, ())
            landed(buffer, block, receive)
            for b in bits:
                push(buffer, block, flip(me, b), send, receive)

    def forward_level(buffer, level, send, receive, steps=None):
        for flips in subsets(bits[:level]):
            for step in range(major) if steps is None else steps:
                block = block_of(step, flips + (bits[level],))
                landed(buffer, block, receive)
                for b in bits[level + 1 :]:
                    push(buffer, block, flip(me, b), send, receive)

    first_slot = me * rows

    def find_child(beam, found):
        origin = parent[beam]
        return tuple(
            jnp.where(origin == first_slot + slot, beam, found[slot]) for slot in range(rows)
        )

    own_copies[0].wait()
    pl.semaphore_wait(barrier, len(greeted))
    push_own(all_q, send_sem.at[0], q_sem)
    own_copies[1].wait()
    product = all_q[me].astype(F32) * own_key[...].astype(F32)
    lane = lax.broadcasted_iota(jnp.int32, (rows, LANES), 1)
    self_rows = jnp.zeros((rows, LANES), F32)
    for head in range(heads):
        total = jnp.sum(
            product[:, head * HEAD_DIM : (head + 1) * HEAD_DIM], axis=1, keepdims=True
        )
        self_rows = jnp.where(lane == head, total * scale, self_rows)
    all_s[me] = self_rows
    own_copies[2].wait()
    own_copies[3].wait()
    push_own(all_s, send_sem.at[1], s_sem)
    push_own(all_vr, send_sem.at[2], vr_sem)
    weight_waits = []
    for number, (source, target) in enumerate(((w_gate, gate), (w_up, up), (w_down, down))):
        depth = target.shape[0]
        part = depth // 4
        for chunk in range(4):
            span = pl.ds(chunk * part, part)
            pltpu.make_async_copy(
                source.at[0, span, :], target.at[span, :], weight_sem.at[number]
            ).start()
        weight_waits.append(pltpu.make_async_copy(target, target, weight_sem.at[number]))

    for copy in small_copies:
        copy.wait()
    child = lax.fori_loop(
        0, parent.shape[0], find_child, tuple(jnp.int32(0) for _ in range(rows))
    )

    places = experts * capacity

    def slot_tables(shape, dimension):
        numbers = lax.broadcasted_iota(jnp.int32, shape, dimension)
        expert_of, rank_of = lax.div(numbers, capacity), lax.rem(numbers, capacity)
        ranks = jnp.zeros(shape, jnp.int32)
        placed, weights = [], []
        for slot in range(rows):
            named = jnp.zeros(shape, jnp.int32)
            weight = jnp.zeros(shape, F32)
            for pick in range(chosen):
                hit = expert_of == route_ids[pick, first_slot + slot]
                named = jnp.where(hit, 1, named)
                weight = weight + jnp.where(hit, route_weights[pick, first_slot + slot], 0.0)
            mine = (named == 1) & (ranks == rank_of)
            placed.append(jnp.where(mine, 1.0, 0.0))
            weights.append(jnp.where(mine, weight, 0.0))
            ranks = ranks + named
        return placed, weights

    placed, _ = slot_tables((places, 1), 0)
    lanes_of_places = -(-places // LANES) * LANES
    _, lane_weights = slot_tables((1, lanes_of_places), 1)
    row_number = lax.broadcasted_iota(jnp.int32, (rows, lanes_of_places), 0)
    combine = jnp.zeros((rows, lanes_of_places), F32)
    for slot in range(rows):
        combine = jnp.where(row_number == slot, lane_weights[slot], combine)

    forward_line(all_q, send_sem.at[0], q_sem)
    forward_line(all_s, send_sem.at[1], s_sem)
    levels = len(bits)
    for level in range(levels):
        if level == 0:
            forward_line(all_vr, send_sem.at[2], vr_sem)
            forward_level(all_q, level, send_sem.at[0], q_sem)
        else:
            forward_level(all_q, level, send_sem.at[0], q_sem)
        forward_level(all_s, level, send_sem.at[1], s_sem)

    head_mask = lax.broadcasted_iota(jnp.int32, (heads, width), 0) == lax.div(
        lax.broadcasted_iota(jnp.int32, (heads, width), 1), HEAD_DIM
    )
    self_mask = lax.broadcasted_iota(jnp.int32, (heads, LANES), 0) == lax.broadcasted_iota(
        jnp.int32, (heads, LANES), 1
    )

    def pick(block, row):
        block = block.astype(F32)
        chosen_row = lax.broadcasted_iota(jnp.int32, block.shape, 0) == row
        return jnp.sum(jnp.where(chosen_row, block, 0.0), axis=0, keepdims=True)

    probs, selfs, denominators = [], [], []
    for slot in range(rows):
        device, row = lax.div(child[slot], rows), lax.rem(child[slot], rows)
        query = pick(all_q[device], row)
        spread_query = jnp.where(head_mask, query, 0.0).astype(BF16)
        key_copies[slot].wait()
        scores = (
            lax.dot_general(
                spread_query,
                keys[slot],
                (((1,), (1,)), ((), ())),
                preferred_element_type=F32,
            )
            * scale
        )
        self_score = jnp.sum(
            jnp.where(self_mask, pick(all_s[device], row), 0.0), axis=1, keepdims=True
        )
        peak = jnp.maximum(jnp.max(scores, axis=1, keepdims=True), self_score)
        expo = jnp.exp(scores - peak)
        self_expo = jnp.exp(self_score - peak)
        denominators.append(jnp.sum(expo, axis=1, keepdims=True) + self_expo)
        probs.append(expo.astype(BF16))
        selfs.append(self_expo.astype(BF16).astype(F32))
    if levels:
        forward_level(all_vr, 0, send_sem.at[2], vr_sem)
    for slot in range(rows):
        value_copies[slot].wait()
        mixed_ref[slot] = jnp.dot(probs[slot], values[slot], preferred_element_type=F32)
    for level in range(1, levels):
        forward_level(all_vr, level, send_sem.at[2], vr_sem)

    gains = gain[...]
    normed = []
    for slot in range(rows):
        device, row = lax.div(child[slot], rows), lax.rem(child[slot], rows)
        new_value = pick(all_vr[device, 0], row)
        residual = pick(all_vr[device, 1], row)
        mixed = (mixed_ref[slot] + selfs[slot] * new_value) / denominators[slot]
        attended = jnp.sum(jnp.where(head_mask, mixed, 0.0), axis=0, keepdims=True)
        hidden = residual + attended.astype(BF16).astype(F32)
        hidden_ref[pl.ds(slot, 1), :] = hidden
        mean = jnp.mean(hidden * hidden, axis=1, keepdims=True)
        row_normed = (hidden * lax.rsqrt(mean + 1e-06) * gains).astype(BF16)
        normed.append(row_normed.astype(F32))
    total = placed[0] * normed[0]
    for slot in range(1, rows):
        total = total + placed[slot] * normed[slot]
    spread[...] = total
    part = width // PIECES
    for piece in range(PIECES):
        columns = pl.ds(piece * part, part)
        for expert in range(experts):
            disp[piece, expert] = spread[pl.ds(expert * capacity, capacity), columns].astype(BF16)
        for step in range(1, count):
            target = other(step)
            pltpu.make_async_remote_copy(
                src_ref=disp.at[piece, lax.div(target, beams)],
                dst_ref=arrived.at[piece, me],
                send_sem=send_sem.at[3 + piece],
                recv_sem=token_sem.at[piece],
                device_id=place(target),
                device_id_type=pl.DeviceIdType.MESH,
            ).start()
        arrived[piece, me] = disp[piece, lax.div(me, beams)]

    def rest_of(buffer, piece):
        return buffer.at[piece, pl.ds(0, count - 1)]

    for piece in range(PIECES):
        rest = rest_of(arrived, piece)
        pltpu.make_async_copy(rest, rest, token_sem.at[piece]).wait()
        for source in range(count):
            tokens[pl.ds(source * capacity, capacity), :] = arrived[piece, source].astype(F32)
        if piece == 0:
            weight_waits[0].wait()
            weight_waits[1].wait()
        span = pl.ds(piece * part, part)
        left = tokens[...].astype(BF16)
        gate_part = jnp.dot(left, gate[span, :], preferred_element_type=F32)
        up_part = jnp.dot(left, up[span, :], preferred_element_type=F32)
        if piece == 0:
            gate_acc[...] = gate_part
            up_acc[...] = up_part
        else:
            gate_acc[...] += gate_part
            up_acc[...] += up_part
    activation = gate_acc[...]
    inner = (activation / (1.0 + jnp.exp(-activation)) * up_acc[...]).astype(BF16)
    weight_waits[2].wait()
    for piece in range(PIECES):
        piece_ref[...] = jnp.dot(
            inner, down[:, piece * part : (piece + 1) * part], preferred_element_type=F32
        )
        for source in range(count):
            outgoing[piece, source] = piece_ref[pl.ds(source * capacity, capacity), :].astype(BF16)
        for step in range(1, count):
            target = other(step)
            pltpu.make_async_remote_copy(
                src_ref=outgoing.at[piece, target],
                dst_ref=returned.at[piece, me],
                send_sem=send_sem.at[3 + PIECES + piece],
                recv_sem=back_sem.at[piece],
                device_id=place(target),
                device_id_type=pl.DeviceIdType.MESH,
            ).start()
        returned[piece, me] = outgoing[piece, me]

    for piece in range(PIECES):
        rest = rest_of(returned, piece)
        pltpu.make_async_copy(rest, rest, back_sem.at[piece]).wait()
        columns = pl.ds(piece * part, part)
        sums = hidden_ref[:, columns]
        for source in range(count):
            block = returned[piece, source].astype(F32)
            for rank in range(capacity):
                at = (source // beams) * capacity + rank
                sums = sums + combine[:, at : at + 1] * block[rank : rank + 1, :]
        out[:, columns] = sums.astype(out.dtype)

    for number, buffer in enumerate((all_q, all_s, all_vr)):
        sent = buffer.at[pl.ds(0, count - 1)]
        pltpu.make_async_copy(sent, sent, send_sem.at[number]).wait()
    for piece in range(PIECES):
        for number, buffer in ((3, arrived), (3 + PIECES, outgoing)):
            sent = rest_of(buffer, piece)
            pltpu.make_async_copy(sent, sent, send_sem.at[number + piece]).wait()


def body(
    queries,
    new_keys,
    new_values,
    resid,
    key_cache,
    value_cache,
    parent,
    route_ids,
    route_weights,
    norm_gain,
    w_gate,
    w_up,
    w_down,
):
    rows, width = queries.shape
    positions = key_cache.shape[1]
    hidden_units = w_gate.shape[2]
    experts, beams = lax.axis_size("expert"), lax.axis_size("beam")
    count = experts * beams
    minor = beams
    while minor < 4 and beams == 1 and experts % (2 * minor) == 0:
        minor *= 2
    capacity = max(2, -(-rows * route_ids.shape[1] // experts))
    heads = width // HEAD_DIM
    part = width // PIECES
    vmem = pltpu.VMEM
    smem = pltpu.SMEM
    any_spec = pl.BlockSpec(memory_space=pl.ANY)
    vmem_spec = pl.BlockSpec(memory_space=pltpu.VMEM)
    dma = pltpu.SemaphoreType.DMA
    return pl.pallas_call(
        functools.partial(layer_kernel, (experts, beams, minor, capacity)),
        out_shape=jax.ShapeDtypeStruct((rows, width), BF16),
        in_specs=[any_spec] * 13,
        out_specs=vmem_spec,
        scratch_shapes=[
            smem(parent.shape, jnp.int32),
            smem(route_ids.shape[::-1], jnp.int32),
            smem(route_weights.shape[::-1], F32),
            vmem((1, width), F32),
            vmem((count, rows, width), BF16),
            vmem((count, rows, LANES), F32),
            vmem((count, 2, rows, width), BF16),
            vmem((rows, width), BF16),
            vmem((rows, positions, width), BF16),
            vmem((rows, positions, width), BF16),
            vmem((width, hidden_units), BF16),
            vmem((width, hidden_units), BF16),
            vmem((hidden_units, width), BF16),
            vmem((rows, heads, width), F32),
            vmem((rows, width), F32),
            vmem((experts * capacity, width), F32),
            vmem((PIECES, experts, capacity, part), BF16),
            vmem((PIECES, count, capacity, part), BF16),
            vmem((count * capacity, part), F32),
            vmem((count * capacity, hidden_units), F32),
            vmem((count * capacity, hidden_units), F32),
            vmem((count * capacity, part), F32),
            vmem((PIECES, count, capacity, part), BF16),
            vmem((PIECES, count, capacity, part), BF16),
            dma((8,)),
            dma((rows,)),
            dma((rows,)),
            dma((3,)),
            dma((3 + 2 * PIECES,)),
            dma((count,)),
            dma((count,)),
            dma((count,)),
            dma((PIECES,)),
            dma((PIECES,)),
        ],
        compiler_params=pltpu.CompilerParams(collective_id=0, has_side_effects=True),
    )(
        parent,
        route_ids.T,
        route_weights.T,
        norm_gain[None, :],
        queries,
        new_keys,
        new_values,
        resid,
        key_cache,
        value_cache,
        w_gate,
        w_up,
        w_down,
    )


def solution(mesh):
    return jax.shard_map(
        body,
        mesh=mesh,
        in_specs=(
            P(("groups", "expert", "beam"), None),
            P(("groups", "expert", "beam"), None),
            P(("groups", "expert", "beam"), None),
            P(("groups", "expert", "beam"), None),
            P(("groups", "expert", "beam"), None, None),
            P(("groups", "expert", "beam"), None, None),
            P("groups"),
            P("groups", None),
            P("groups", None),
            P(),
            P("expert", None, "beam"),
            P("expert", None, "beam"),
            P("expert", "beam", None),
        ),
        out_specs=P(("groups", "expert", "beam"), None),
        check_vma=False,
    )
```
